128 devices in a mesh: col: 8 (over x, z_lo), row: 16 (over y, z_hi, core).
Axes of the slice: x: 4, y: 4, z: 4 (z_hi: 2, z_lo: 2; z = z_hi * 2 + z_lo), core: 2. Of those that a mesh axis runs over, the one named last changes fastest.
Arguments:
- data: bfloat16 [32768, 8192], P('row', 'col'), may hold values from -6 to 6
- column_scale: float32 [8192], P('col'), may hold values from 0.25 to 4
- keep_mask: int32 [32768, 8192], P('row', 'col'), may hold values 0 or 1
Outputs:
- band: float32 [8192, 5, 1024], P('col', None, 'row')
The draws below stay inside these ranges and needn't reach their ends.
All inputs are finite; a program needn't handle non-finite values. No bound on the sum of `keep_mask` on one device may be relied on, other than what follows from the above.
Results may differ from the reference program's by a relative error of at most 0.0012.
Values may be sent and summed in bfloat16 or wider, within the bound.
A program may use at most 128 MiB of HBM per device.

```python
import math
import jax
import jax.numpy as jnp
from jax import lax

COLS = 8192
ROWS = 32768
PANEL = 1024
HALF = 5
N_COL = 8


def with_ends(values, key, low, top_value):
    shape = values.shape
    index_at = [jax.random.randint(jax.random.fold_in(key, axis), (), 0, shape[axis]) for axis in range(len(shape))]
    values = values.at[tuple(index_at)].set(low)
    longest = shape.index(max(shape))
    index_at[longest] = (index_at[longest] + 1) % shape[longest]
    return values.at[tuple(index_at)].set(top_value)


def levels(key, shape, shards, least, top_value):
    level, own = 1.0, jax.random.fold_in(key, 6)
    for dim, blocks in shards:
        steps = jnp.exp(jax.random.uniform(jax.random.fold_in(own, dim), (blocks,), jnp.float32, least / len(shards), top_value / len(shards)))
        level = level * jnp.repeat(steps, shape[dim] // blocks).reshape([-1 if axis == dim else 1 for axis in range(len(shape))])
    return level


def normal_values(key, dims, deviation, reach, cuts=(), held_as=jnp.bfloat16):
    drawn = jax.random.normal(key, dims, jnp.float32) * deviation
    if len(cuts) > 0:
        drawn = levels(key, dims, cuts, -0.22, 0.18) * drawn
    return jnp.clip(drawn, min=-reach, max=reach).astype(held_as)


def setup_inputs(seed: int = 0) -> dict:
    splits = jax.random.split(jax.random.key(seed), 4)
    data = normal_values(splits[0], (ROWS, COLS), 1.0, 6.0, ((0, 16), (1, 8)))
    column_scale = jnp.clip(jnp.exp(math.log(4.0) - 2.7725887 * jax.random.uniform(splits[1], (COLS,), jnp.float32) ** levels(splits[1], (COLS,), ((0, 8),), -0.2, 0.2)), 0.25, 4.0)
    keep_mask = with_ends((jax.random.randint(splits[2], (ROWS, COLS), 0, 4) < 3).astype(jnp.int32), jax.random.fold_in(splits[2], 1), 0, 1)
    return {"data": data, "column_scale": column_scale, "keep_mask": keep_mask}


def reference(data, column_scale, keep_mask):
    values = data.astype(jnp.float32) * column_scale[None, :]
    colsq = lax.optimization_barrier(jnp.sum(values * values, axis=0))
    divisor = jnp.minimum(jnp.sqrt(colsq + 1.0), jnp.sqrt(jnp.float32(ROWS)))
    scaled = (keep_mask.astype(jnp.float32) * values / divisor[None, :]).astype(jnp.bfloat16)
    wide = scaled.astype(jnp.float32)
    blocks = []
    for panel_index in range(N_COL):
        left = wide[:, panel_index * PANEL:(panel_index + 1) * PANEL]
        rolled = jnp.roll(wide, -panel_index * PANEL, axis=1)[:, :HALF * PANEL]
        tile = jnp.dot(left.T, rolled, precision=lax.Precision.HIGHEST, preferred_element_type=jnp.float32)
        blocks.append(tile.reshape(PANEL, HALF, PANEL))
    return jnp.concatenate(blocks, axis=0)
```

```python
import jax
import jax.numpy as jnp
from jax import lax
from jax.experimental import pallas as pl
from jax.experimental.pallas import tpu as pltpu
from jax.sharding import Mesh
from jax.sharding import PartitionSpec as P

AXES = ("x", "zl", "y", "zh", "co")
ROW = ("y", "zh", "co")
NS = 4
NT = 2

PHASES = (
    [(0, s, t) for s in range(4) for t in range(2)],
    [(1, 0, 0), (1, 0, 1)],
    [(1, 1, 0), (1, 1, 1), (3, 0, 0), (3, 1, 0)],
    [(1, 2, 0), (1, 2, 1), (3, 2, 0), (2, 0, 0), (2, 0, 1), (4, 0, 0)],
    [(1, 3, 0), (1, 3, 1), (3, 3, 0)] + [(3, s, 1) for s in range(4)] + [(4, 0, 1)],
    [(2, 1, 0), (2, 1, 1), (4, 1, 0), (4, 1, 1)],
    [(2, 2, 0), (2, 2, 1), (4, 2, 0), (4, 2, 1)],
    [(2, 3, 0), (2, 3, 1), (4, 3, 0), (4, 3, 1)],
)
ITEMS = [item for phase in PHASES for item in phase]
N = len(ITEMS)
RING = 8
CODES = [b * 8 + s * 2 + t for b, s, t in ITEMS]
WORDS = [sum(c << (6 * i) for i, c in enumerate(CODES[g:g + 5])) for g in range(0, N, 5)]


def item_of(n):
    group = n // 5
    word = sum(jnp.where(group == g, jnp.int32(w), 0) for g, w in enumerate(WORDS))
    code = lax.shift_right_logical(word, 6 * (n % 5)) % 64
    return code // 8, (code // 2) % 4, code % 2


def kernel(p_hbm, pt_hbm, out_ref, lb, rb, rel, part, d2, y1, y2, zs, z1, za,
           in_sem, xs, xr, ds, dr, y1s, y1r, y2s, y2r, z1s, z1r, zas, zar):
    x, zl, y, zh, co = (lax.axis_index(a) for a in AXES)
    xm, xp = (x + 3) % 4, (x + 1) % 4
    ym, yp, yo = (y + 3) % 4, (y + 1) % 4, (y + 2) % 4

    def remote(src, dst, send, recv, dev):
        return pltpu.make_async_remote_copy(
            src_ref=src, dst_ref=dst, send_sem=send, recv_sem=recv,
            device_id=dev, device_id_type=pl.DeviceIdType.MESH)

    loads = []
    for s in range(NS):
        loads.append(pltpu.make_async_copy(pt_hbm.at[s], rb.at[s], in_sem.at[s]))
    for t in range(NT):
        loads.append(pltpu.make_async_copy(
            p_hbm.at[:, t * 512:(t + 1) * 512], lb.at[t], in_sem.at[NS + t]))
    for c in loads:
        c.start()

    barrier = pltpu.get_barrier_semaphore()
    others = [(x, zl, y, zh, 1 - co), (x, zl, yp, zh, co), (x, zl, ym, zh, co),
              (x, zl, y, 1 - zh, co), (x, 1 - zl, y, zh, co), (x, 1 - zl, y, 1 - zh, co),
              (xm, zl, y, zh, co), (xp, zl, y, zh, co)]
    for dev in others:
        pl.semaphore_signal(barrier, inc=1, device_id=dev, device_id_type=pl.DeviceIdType.MESH)
    pl.semaphore_wait(barrier, len(others))
    for c in loads:
        c.wait()

    to_xm, to_xp, to_z = (xm, zl, y, zh, co), (xp, zl, y, zh, co), (x, 1 - zl, y, zh, co)
    flow = [remote(rb.at[s], rb.at[4 + s], xs.at[s], xr.at[s], to_xm) for s in range(4)]
    flow += [
        remote(rb.at[0], rel.at[pl.ds(0, 256)], xs.at[4], xr.at[4], to_xp),
        remote(rb.at[1], rel.at[pl.ds(256, 256)], xs.at[5], xr.at[5], to_xp),
        remote(rb.at[3, pl.ds(64, 192)], rel.at[pl.ds(512, 192)], xs.at[6], xr.at[6], to_xp),
    ]
    flow += [remote(lb.at[t], lb.at[NT + t], xs.at[7 + t], xr.at[7 + t], to_z) for t in range(NT)]
    flow += [
        remote(rb.at[6], rb.at[10], xs.at[9], xr.at[9], to_xm),
        remote(rb.at[7, pl.ds(0, 64)], rb.at[11, pl.ds(0, 64)], xs.at[10], xr.at[10], to_xm),
        remote(rel.at[pl.ds(0, 256)], rb.at[8], xs.at[11], xr.at[11], to_xp),
        remote(rel.at[pl.ds(256, 256)], rb.at[9], xs.at[12], xr.at[12], to_xp),
        remote(rel.at[pl.ds(512, 192)], rb.at[11, pl.ds(64, 192)], xs.at[13], xr.at[13], to_xp),
    ]
    for f in (0, 4, 7, 1, 5, 8, 2, 3):
        flow[f].start()

    other_half = (1 - co) * 128
    own_half = co * 128

    def d2_copy(n, slot):
        return remote(part.at[slot, pl.ds(other_half, 128)], d2.at[n], ds.at[slot], dr.at[n],
                      (x, zl, y, zh, 1 - co))

    def y1_copies(n, slot):
        base = own_half + yo * 32
        return (remote(part.at[slot, pl.ds(base, 16)], y1.at[n, 0], y1s.at[slot, 0], y1r.at[n, 0],
                       (x, zl, yp, zh, co)),
                remote(part.at[slot, pl.ds(base + 16, 16)], y1.at[n, 1], y1s.at[slot, 1],
                       y1r.at[n, 1], (x, zl, ym, zh, co)))

    def y2_copies(n, slot):
        return (remote(part.at[slot, pl.ds(own_half + yp * 32, 32)], y2.at[n, 0],
                       y2s.at[slot, 0], y2r.at[n, 0], (x, zl, yp, zh, co)),
                remote(part.at[slot, pl.ds(own_half + ym * 32, 32)], y2.at[n, 1],
                       y2s.at[slot, 1], y2r.at[n, 1], (x, zl, ym, zh, co)))

    def z1_copy(n, left):
        return remote(zs.at[n, pl.ds((1 - zh) * 16, 16)], z1.at[n], z1s.at[n], z1r.at[n],
                      (x, (zl + left) % 2, y, 1 - zh, co))

    def za_copy(n):
        return remote(zs.at[n, pl.ds(zh * 16, 16)], za.at[n], zas.at[n], zar.at[n], to_z)

    def multiply(first, count):
        @pl.loop(first, first + count)
        def _(n):
            b, s, t = item_of(n)
            left = b // 3
            right = b - 3 * left + left * (1 - zl)
            slot = n % RING
            part[slot] = jnp.dot(rb[right * 4 + s], lb[left * NT + t],
                                 preferred_element_type=jnp.float32)
            d2_copy(n, slot).start()

    def add_core(first, count):
        @pl.loop(first, first + count)
        def _(n):
            slot = n % RING
            d2_copy(n, slot).wait()
            rows = pl.ds(own_half, 128)
            part[slot, rows] = part[slot, rows] + d2[n]
            for c in y1_copies(n, slot):
                c.start()

    def add_y1(first, count):
        @pl.loop(first, first + count)
        def _(n):
            slot = n % RING
            for c in y1_copies(n, slot):
                c.wait()
            rows = pl.ds(own_half + yp * 32, 16)
            part[slot, rows] = part[slot, rows] + y1[n, 0]
            rows = pl.ds(own_half + ym * 32 + 16, 16)
            part[slot, rows] = part[slot, rows] + y1[n, 1]
            for c in y2_copies(n, slot):
                c.start()

    def add_y2(first, count):
        @pl.loop(first, first + count)
        def _(n):
            slot = n % RING
            b, _s, _t = item_of(n)
            left = b // 3
            for c in y2_copies(n, slot):
                c.wait()
            zs[n] = part[slot, pl.ds(own_half + y * 32, 32)] + y2[n, 0] + y2[n, 1]
            z1_copy(n, left).start()

            @pl.when(left == 1)
            def _():
                za_copy(n).start()

    def finish(first, count):
        @pl.loop(first, first + count)
        def _(n):
            b, s, t = item_of(n)
            left = b // 3
            z1_copy(n, left).wait()
            rows = pl.ds(pl.multiple_of(s * 16, 16), 16)
            lanes = pl.ds(pl.multiple_of(t * 512, 512), 512)

            @pl.when(left == 1)
            def _():
                za_copy(n).wait()
                out_ref[2 * (b - 3) + 1, rows, lanes] = za[n] + z1[n]

            @pl.when(left == 0)
            def _():
                out_ref[2 * b, rows, lanes] = zs[n, pl.ds(zh * 16, 16)] + z1[n]

    def arrive(*numbers):
        for f in numbers:
            flow[f].wait_recv()

    def start(*numbers):
        for f in numbers:
            flow[f].start()

    first = 0
    for number, phase in enumerate(PHASES):
        if number == 1:
            arrive(0, 4)
            start(11, 6)
        elif number == 2:
            arrive(1, 5, 7)
            start(12)
        elif number == 3:
            arrive(2)
            start(9)
            arrive(11)
        elif number == 4:
            arrive(3, 6, 8)
            start(10, 13)
        elif number == 5:
            arrive(12)
        elif number == 6:
            arrive(9)
        elif number == 7:
            arrive(10, 13)
        count = len(phase)
        multiply(first, count)
        add_core(first, count)
        add_y1(first, count)
        add_y2(first, count)
        first += count
    finish(0, N)
    for c in flow:
        c.wait_send()


def gram(panel, panel_t):
    dma = pltpu.SemaphoreType.DMA
    f32, bf16 = jnp.float32, jnp.bfloat16
    return pl.pallas_call(
        kernel,
        out_shape=jax.ShapeDtypeStruct((5, 64, 1024), f32),
        in_specs=[pl.BlockSpec(memory_space=pl.ANY)] * 2,
        out_specs=pl.BlockSpec(memory_space=pltpu.VMEM),
        scratch_shapes=[
            pltpu.VMEM((2 * NT, 2048, 512), bf16),
            pltpu.VMEM((12, 256, 2048), bf16),
            pltpu.VMEM((704, 2048), bf16),
            pltpu.VMEM((RING, 256, 512), f32),
            pltpu.VMEM((N, 128, 512), f32),
            pltpu.VMEM((N, 2, 16, 512), f32),
            pltpu.VMEM((N, 2, 32, 512), f32),
            pltpu.VMEM((N, 32, 512), f32),
            pltpu.VMEM((N, 16, 512), f32),
            pltpu.VMEM((N, 16, 512), f32),
            dma((NS + NT,)), dma((14,)), dma((14,)),
            dma((RING,)), dma((N,)),
            dma((RING, 2)), dma((N, 2)), dma((RING, 2)), dma((N, 2)),
            dma((N,)), dma((N,)), dma((N,)), dma((N,)),
        ],
        compiler_params=pltpu.CompilerParams(
            collective_id=0, has_side_effects=True, vmem_limit_bytes=67043328),
    )(panel, panel_t)


def of_everyone(value, axis):
    peers = lax.axis_size(axis)
    return lax.all_to_all(
        jnp.broadcast_to(value[None], (peers, *value.shape)), axis, 0, 0, tiled=True
    ).sum(axis=0)


def on_device(data, column_scale, keep_mask):
    values = data.astype(jnp.float32) * column_scale[None, :]
    colsq = of_everyone(jnp.sum(values * values, axis=0), ROW)
    total_rows = data.shape[0] * lax.axis_size(ROW)
    divisor = jnp.minimum(jnp.sqrt(colsq + 1.0), jnp.sqrt(jnp.float32(total_rows)))
    scaled = (keep_mask.astype(jnp.float32) * values / divisor[None, :]).astype(jnp.bfloat16)
    rows = scaled.T.reshape(4, 2, 2, 4, 16, -1).transpose(3, 2, 0, 1, 4, 5)
    band = gram(scaled, rows.reshape(4, 256, -1))
    return band.transpose(2, 0, 1)


def solution(mesh):
    split = Mesh(mesh.devices.reshape(4, 2, 4, 2, 2), AXES)
    return jax.shard_map(
        on_device,
        mesh=split,
        in_specs=(P(ROW, ("x", "zl")), P(("x", "zl")), P(ROW, ("x", "zl"))),
        out_specs=P(("x", "zl"), None, ROW),
        check_vma=False,
    )
```

```python
import jax
import jax.numpy as jnp
from jax import lax
from jax.experimental import pallas as pl
from jax.experimental.pallas import tpu as pltpu
from jax.sharding import Mesh
from jax.sharding import PartitionSpec as P

AXES = ("x", "zl", "y", "zh", "co")
ROW = ("y", "zh", "co")
NS = 4
NT = 2

PHASES = (
    [(0, 0, 0), (0, 0, 1), (0, 1, 0), (0, 1, 1)],
    [(0, 2, 0), (0, 2, 1), (0, 3, 0), (0, 3, 1)],
    [(1, 0, 0), (1, 0, 1)],
    [(1, 1, 0), (1, 1, 1), (3, 0, 0), (3, 1, 0)],
    [(2, 0, 0), (2, 0, 1), (4, 0, 0)],
    [(1, 2, 0), (1, 2, 1), (3, 2, 0)],
    [(1, 3, 0), (1, 3, 1), (3, 3, 0), (3, 3, 1)],
    [(3, 0, 1), (3, 1, 1), (3, 2, 1), (4, 0, 1)],
    [(2, 1, 0), (2, 1, 1), (4, 1, 0), (4, 1, 1)],
    [(2, 2, 0), (2, 2, 1), (4, 2, 0), (4, 2, 1)],
    [(2, 3, 0), (2, 3, 1), (4, 3, 0), (4, 3, 1)],
)
ITEMS = [item for phase in PHASES for item in phase]
N = len(ITEMS)
RING = 8
STEP = 256
CODES = [b * 8 + s * 2 + t for b, s, t in ITEMS]
WORDS = [sum(c << (6 * i) for i, c in enumerate(CODES[g:g + 5])) for g in range(0, N, 5)]


def item_of(n):
    group = n // 5
    word = sum(jnp.where(group == g, jnp.int32(w), 0) for g, w in enumerate(WORDS))
    code = lax.shift_right_logical(word, 6 * (n % 5)) % 64
    return code // 8, (code // 2) % 4, code % 2


def kernel(data_hbm, mask_hbm, scale_ref, out_ref, lb, rb, rel, part, d2, y1, y2, zs, z1, za,
           mask, cs, wcol, in_sem, css, csr, xs, xr, ds, dr, y1s, y1r, y2s, y2r,
           z1s, z1r, zas, zar):
    x, zl, y, zh, co = (lax.axis_index(a) for a in AXES)
    xm, xp = (x + 3) % 4, (x + 1) % 4
    ym, yp, yo = (y + 3) % 4, (y + 1) % 4, (y + 2) % 4
    me = y * 4 + zh * 2 + co
    f32, bf16 = jnp.float32, jnp.bfloat16

    def remote(src, dst, send, recv, dev):
        return pltpu.make_async_remote_copy(
            src_ref=src, dst_ref=dst, send_sem=send, recv_sem=recv,
            device_id=dev, device_id_type=pl.DeviceIdType.MESH)

    def loads(i):
        rows = pl.ds(pl.multiple_of(i * STEP, STEP), STEP)
        return [pltpu.make_async_copy(mask_hbm.at[rows], mask.at[rows], in_sem.at[i, NT])] + [
            pltpu.make_async_copy(data_hbm.at[rows, t * 512:(t + 1) * 512], lb.at[t, rows],
                                  in_sem.at[i, t]) for t in range(NT)]

    @pl.loop(0, 2048 // STEP)
    def _(i):
        for c in loads(i):
            c.start()

    def row_peer(r):
        return (x, zl, r // 4, (r // 2) % 2, r % 2)

    barrier = pltpu.get_barrier_semaphore()
    others = [row_peer((me + d) % 16) for d in range(1, 16)]
    others += [(x, 1 - zl, y, zh, co), (x, 1 - zl, y, 1 - zh, co),
               (xm, zl, y, zh, co), (xp, zl, y, zh, co)]
    for dev in others:
        pl.semaphore_signal(barrier, inc=1, device_id=dev, device_id_type=pl.DeviceIdType.MESH)

    cs[16] = jnp.zeros((8, 1024), f32)

    @pl.loop(0, 2048 // STEP)
    def _(i):
        for c in loads(i):
            c.wait()
        rows = pl.ds(pl.multiple_of(i * STEP, STEP), STEP)
        for t in range(NT):
            lanes = slice(t * 512, (t + 1) * 512)
            given = lb[t, rows].astype(f32)
            values = given * scale_ref[:, lanes]
            cs[16, :, lanes] += (values * values).reshape(STEP // 8, 8, 512).sum(axis=0)
            kept = (given * mask[rows, lanes].astype(f32)).astype(bf16)
            lb[t, rows] = kept
            turned = kept.T
            for g in range(32):
                j = t * 32 + g
                py, ph, pc, s = j // 16, (j // 8) % 2, (j // 4) % 2, j % 4
                rb[s, pl.ds(pc * 128 + py * 32 + ph * 16, 16), rows] = turned[g * 16:(g + 1) * 16]

    cs[me] = jnp.broadcast_to(cs[16].sum(axis=0, keepdims=True), (8, 1024))
    pl.semaphore_wait(barrier, len(others))

    def cs_copy(slot, peer):
        return remote(cs.at[slot], cs.at[slot], css.at[peer], csr.at[slot], row_peer(peer))

    @pl.loop(1, 16)
    def _(d):
        cs_copy(me, (me + d) % 16).start()

    @pl.loop(1, 16)
    def _(d):
        cs_copy((me + d) % 16, (me + d) % 16).wait_recv()

    colsq = cs[0]
    for r in range(1, 16):
        colsq = colsq + cs[r]
    divisor = jnp.minimum(jnp.sqrt(colsq + 1.0), jnp.sqrt(jnp.float32(32768.0)))
    weight = scale_ref[...] / divisor[0:1]
    wcol[...] = jnp.broadcast_to(weight, (128, 1024)).T

    def scale_rb(s):
        @pl.loop(0, 16)
        def _(r):
            pc, py, ph = r // 8, (r // 2) % 4, r % 2
            j = pl.multiple_of(py * 256 + ph * 128 + pc * 64 + s * 16, 16)
            rows = pl.ds(pl.multiple_of(r * 16, 16), 16)
            by = wcol[pl.ds(j, 16), 0:1]
            rb[s, rows] = (rb[s, rows].astype(f32) * by).astype(bf16)

    def scale_lb(t):
        by = weight[:, t * 512:(t + 1) * 512]

        @pl.loop(0, 16)
        def _(i):
            rows = pl.ds(pl.multiple_of(i * 128, 128), 128)
            lb[t, rows] = (lb[t, rows].astype(f32) * by).astype(bf16)

    to_xm, to_xp, to_z = (xm, zl, y, zh, co), (xp, zl, y, zh, co), (x, 1 - zl, y, zh, co)
    flow = [remote(rb.at[s], rb.at[4 + s], xs.at[s], xr.at[s], to_xm) for s in range(4)]
    flow += [
        remote(rb.at[0], rel.at[pl.ds(0, 256)], xs.at[4], xr.at[4], to_xp),
        remote(rb.at[1], rel.at[pl.ds(256, 256)], xs.at[5], xr.at[5], to_xp),
        remote(rb.at[3, pl.ds(64, 192)], rel.at[pl.ds(512, 192)], xs.at[6], xr.at[6], to_xp),
    ]
    flow += [remote(lb.at[t], lb.at[NT + t], xs.at[7 + t], xr.at[7 + t], to_z) for t in range(NT)]
    flow += [
        remote(rb.at[6], rb.at[10], xs.at[9], xr.at[9], to_xm),
        remote(rb.at[7, pl.ds(0, 64)], rb.at[11, pl.ds(0, 64)], xs.at[10], xr.at[10], to_xm),
        remote(rel.at[pl.ds(0, 256)], rb.at[8], xs.at[11], xr.at[11], to_xp),
        remote(rel.at[pl.ds(256, 256)], rb.at[9], xs.at[12], xr.at[12], to_xp),
        remote(rel.at[pl.ds(512, 192)], rb.at[11, pl.ds(64, 192)], xs.at[13], xr.at[13], to_xp),
    ]
    scale_rb(0)
    flow[0].start()
    flow[4].start()
    scale_lb(0)
    flow[7].start()
    scale_rb(1)
    flow[1].start()
    scale_lb(1)
    flow[8].start()
    for s in (2, 3):
        scale_rb(s)
        flow[s].start()

    other_half = (1 - co) * 128
    own_half = co * 128

    def d2_copy(n, slot):
        return remote(part.at[slot, pl.ds(other_half, 128)], d2.at[n], ds.at[slot], dr.at[n],
                      (x, zl, y, zh, 1 - co))

    def y1_copies(n, slot):
        base = own_half + yo * 32
        return (remote(part.at[slot, pl.ds(base, 16)], y1.at[n, 0], y1s.at[slot, 0], y1r.at[n, 0],
                       (x, zl, yp, zh, co)),
                remote(part.at[slot, pl.ds(base + 16, 16)], y1.at[n, 1], y1s.at[slot, 1],
                       y1r.at[n, 1], (x, zl, ym, zh, co)))

    def y2_copies(n, slot):
        return (remote(part.at[slot, pl.ds(own_half + yp * 32, 32)], y2.at[n, 0],
                       y2s.at[slot, 0], y2r.at[n, 0], (x, zl, yp, zh, co)),
                remote(part.at[slot, pl.ds(own_half + ym * 32, 32)], y2.at[n, 1],
                       y2s.at[slot, 1], y2r.at[n, 1], (x, zl, ym, zh, co)))

    def z1_copy(n, left):
        return remote(zs.at[n, pl.ds((1 - zh) * 16, 16)], z1.at[n], z1s.at[n], z1r.at[n],
                      (x, (zl + left) % 2, y, 1 - zh, co))

    def za_copy(n):
        return remote(zs.at[n, pl.ds(zh * 16, 16)], za.at[n], zas.at[n], zar.at[n], to_z)

    def multiply(first, count):
        @pl.loop(first, first + count)
        def _(n):
            b, s, t = item_of(n)
            left = b // 3
            right = b - 3 * left + left * (1 - zl)
            slot = n % RING
            part[slot] = jnp.dot(rb[right * 4 + s], lb[left * NT + t],
                                 preferred_element_type=jnp.float32)
            d2_copy(n, slot).start()

    def add_core(first, count):
        @pl.loop(first, first + count)
        def _(n):
            slot = n % RING
            d2_copy(n, slot).wait()
            rows = pl.ds(own_half, 128)
            part[slot, rows] = part[slot, rows] + d2[n]
            for c in y1_copies(n, slot):
                c.start()

    def add_y1(first, count):
        @pl.loop(first, first + count)
        def _(n):
            slot = n % RING
            for c in y1_copies(n, slot):
                c.wait()
            rows = pl.ds(own_half + yp * 32, 16)
            part[slot, rows] = part[slot, rows] + y1[n, 0]
            rows = pl.ds(own_half + ym * 32 + 16, 16)
            part[slot, rows] = part[slot, rows] + y1[n, 1]
            for c in y2_copies(n, slot):
                c.start()

    def add_y2(first, count):
        @pl.loop(first, first + count)
        def _(n):
            slot = n % RING
            b, _s, _t = item_of(n)
            left = b // 3
            for c in y2_copies(n, slot):
                c.wait()
            zs[n] = part[slot, pl.ds(own_half + y * 32, 32)] + y2[n, 0] + y2[n, 1]
            z1_copy(n, left).start()

            @pl.when(left == 1)
            def _():
                za_copy(n).start()

    def finish(first, count):
        @pl.loop(first, first + count)
        def _(n):
            b, s, t = item_of(n)
            left = b // 3
            z1_copy(n, left).wait()
            rows = pl.ds(pl.multiple_of(s * 16, 16), 16)
            lanes = pl.ds(pl.multiple_of(t * 512, 512), 512)

            @pl.when(left == 1)
            def _():
                za_copy(n).wait()
                out_ref[2 * (b - 3) + 1, rows, lanes] = za[n] + z1[n]

            @pl.when(left == 0)
            def _():
                out_ref[2 * b, rows, lanes] = zs[n, pl.ds(zh * 16, 16)] + z1[n]

    def arrive(*numbers):
        for f in numbers:
            flow[f].wait_recv()

    def start(*numbers):
        for f in numbers:
            flow[f].start()

    first, before = 0, None
    for number, phase in enumerate(PHASES):
        if number == 2:
            arrive(4, 0)
            start(11, 5)
        elif number == 3:
            arrive(1, 7)
        elif number == 4:
            arrive(11)
        elif number == 5:
            arrive(5)
            start(12, 6)
            arrive(2)
            start(9)
        elif number == 6:
            arrive(3, 8)
            start(10)
        elif number == 8:
            arrive(12)
        elif number == 9:
            arrive(6)
            start(13)
            arrive(9)
        elif number == 10:
            arrive(10, 13)
        count = len(phase)
        multiply(first, count)
        add_core(first, count)
        if before is not None:
            add_y2(*before)
        add_y1(first, count)
        before = (first, count)
        first += count
    add_y2(*before)
    finish(0, N)
    for c in flow:
        c.wait_send()

    @pl.loop(1, 16)
    def _(d):
        cs_copy(me, (me + d) % 16).wait_send()


def on_device(data, column_scale, keep_mask):
    dma = pltpu.SemaphoreType.DMA
    f32, bf16 = jnp.float32, jnp.bfloat16
    band = pl.pallas_call(
        kernel,
        out_shape=jax.ShapeDtypeStruct((5, 64, 1024), f32),
        in_specs=[pl.BlockSpec(memory_space=pl.ANY)] * 2
        + [pl.BlockSpec(memory_space=pltpu.VMEM)],
        out_specs=pl.BlockSpec(memory_space=pltpu.VMEM),
        scratch_shapes=[
            pltpu.VMEM((2 * NT, 2048, 512), bf16),
            pltpu.VMEM((12, 256, 2048), bf16),
            pltpu.VMEM((704, 2048), bf16),
            pltpu.VMEM((RING, 256, 512), f32),
            pltpu.VMEM((N, 128, 512), f32),
            pltpu.VMEM((N, 2, 16, 512), f32),
            pltpu.VMEM((N, 2, 32, 512), f32),
            pltpu.VMEM((N, 32, 512), f32),
            pltpu.VMEM((N, 16, 512), f32),
            pltpu.VMEM((N, 16, 512), f32),
            pltpu.VMEM((2048, 1024), jnp.int32),
            pltpu.VMEM((17, 8, 1024), f32),
            pltpu.VMEM((1024, 128), f32),
            dma((2048 // STEP, NT + 1)), dma((16,)), dma((16,)), dma((14,)), dma((14,)),
            dma((RING,)), dma((N,)),
            dma((RING, 2)), dma((N, 2)), dma((RING, 2)), dma((N, 2)),
            dma((N,)), dma((N,)), dma((N,)), dma((N,)),
        ],
        compiler_params=pltpu.CompilerParams(
            collective_id=0, has_side_effects=True, vmem_limit_bytes=67043328),
    )(data, keep_mask, column_scale.reshape(1, 1024))
    return band.transpose(2, 0, 1)


def solution(mesh):
    split = Mesh(mesh.devices.reshape(4, 2, 4, 2, 2), AXES)
    return jax.shard_map(
        on_device,
        mesh=split,
        in_specs=(P(ROW, ("x", "zl")), P(("x", "zl")), P(ROW, ("x", "zl"))),
        out_specs=P(("x", "zl"), None, ROW),
        check_vma=False,
    )
```

```python
import re

import jax
import jax.numpy as jnp
from jax import lax
from jax.experimental import pallas as pl
from jax.experimental.pallas import tpu as pltpu
from jax.sharding import Mesh
from jax.sharding import PartitionSpec as P

AXES = ("x", "zl", "y", "zh", "co")
ROW = ("y", "zh", "co")
NS = 4
NT = 2

PHASES = (
    [(0, 0, 0), (0, 0, 1), (0, 1, 0), (0, 1, 1)],
    [(0, 2, 0), (0, 2, 1), (0, 3, 0), (0, 3, 1)],
    [(1, 0, 0), (1, 0, 1)],
    [(1, 1, 0), (1, 1, 1)],
    [(3, 0, 0), (3, 1, 0)],
    [(2, 0, 0), (2, 0, 1), (4, 0, 0)],
    [(1, 2, 0), (1, 2, 1), (3, 2, 0)],
    [(1, 3, 0), (1, 3, 1), (3, 3, 0)],
    [(3, 0, 1), (3, 1, 1), (3, 2, 1), (3, 3, 1)],
    [(4, 0, 1), (2, 1, 0), (2, 1, 1)],
    [(4, 1, 0), (4, 1, 1)],
    [(2, 2, 0), (2, 2, 1), (4, 2, 0), (4, 2, 1)],
    [(4, 3, 0), (4, 3, 1)],
    [(2, 3, 0), (2, 3, 1)],
)
ITEMS = [item for phase in PHASES for item in phase]
N = len(ITEMS)
RING = 16
NARROW = 9
WIDE = sum(len(phase) for phase in PHASES[:NARROW])
STEP = 256
CODES = [b * 8 + s * 2 + t for b, s, t in ITEMS]
WORDS = [sum(c << (6 * i) for i, c in enumerate(CODES[g:g + 5])) for g in range(0, N, 5)]


def item_of(n):
    group = n // 5
    word = sum(jnp.where(group == g, jnp.int32(w), 0) for g, w in enumerate(WORDS))
    code = lax.shift_right_logical(word, 6 * (n % 5)) % 64
    return code // 8, (code // 2) % 4, code % 2


def kernel(data_hbm, mask_hbm, scale_ref, out_near, out_far, lb, rb, lraw, rraw, rel, part, d2, y1, y2,
           h1, g1, h2, g2, zs, mask, acc, cs, cr, wrow, wcol, in_sem, css, csr, ws, wr, xs, xr,
           ds, dr, y1s, y1r, y2s, y2r, z1s, z1r, zas, zar):
    x, zl, y, zh, co = (lax.axis_index(a) for a in AXES)
    xm, xp = (x + 3) % 4, (x + 1) % 4
    xo = (x + 2) % 4
    ym, yp, yo = (y + 3) % 4, (y + 1) % 4, (y + 2) % 4
    f32, bf16 = jnp.float32, jnp.bfloat16

    def remote(src, dst, send, recv, dev):
        return pltpu.make_async_remote_copy(
            src_ref=src, dst_ref=dst, send_sem=send, recv_sem=recv,
            device_id=dev, device_id_type=pl.DeviceIdType.MESH)

    def load_mask(i):
        rows = pl.ds(pl.multiple_of(i * STEP, STEP), STEP)
        return pltpu.make_async_copy(mask_hbm.at[rows], mask.at[i % 3], in_sem.at[i, NT])

    def load_data(i):
        rows = pl.ds(pl.multiple_of(i * STEP, STEP), STEP)
        return [pltpu.make_async_copy(data_hbm.at[rows, t * 512:(t + 1) * 512],
                                      lraw.at[t, rows], in_sem.at[i, t]) for t in range(NT)]

    @pl.loop(0, 2048 // STEP)
    def _(i):
        for c in load_data(i):
            c.start()

        @pl.when(i < 3)
        def _():
            load_mask(i).start()

    barrier = pltpu.get_barrier_semaphore()
    others = [(x, zl, y, zh, 1 - co), (x, zl, yp, zh, co), (x, zl, ym, zh, co),
              (x, zl, y, 1 - zh, co), (x, 1 - zl, y, zh, co), (x, 1 - zl, y, 1 - zh, co),
              (xm, zl, y, zh, co), (xp, zl, y, zh, co), (xo, zl, y, zh, co)]
    for dev in others:
        pl.semaphore_signal(barrier, inc=1, device_id=dev, device_id_type=pl.DeviceIdType.MESH)

    acc[...] = jnp.zeros((8, 1024), f32)

    @pl.loop(0, 2048 // STEP)
    def _(i):
        load_mask(i).wait()
        for c in load_data(i):
            c.wait()
        rows = pl.ds(pl.multiple_of(i * STEP, STEP), STEP)
        for t in range(NT):
            lanes = slice(t * 512, (t + 1) * 512)
            given = lraw[t, rows].astype(f32)
            values = given * scale_ref[:, lanes]
            acc[:, lanes] += (values * values).reshape(STEP // 8, 8, 512).sum(axis=0)
            kept = (given * mask[i % 3, :, lanes].astype(f32)).astype(bf16)
            lraw[t, rows] = kept
            turned = kept.T
            for g in range(32):
                j = t * 32 + g
                py, ph, pc, s = j // 16, (j // 8) % 2, (j // 4) % 2, j % 4
                rraw[s, pl.ds(pc * 128 + py * 32 + ph * 16, 16), rows] = turned[g * 16:(g + 1) * 16]

        @pl.when(i + 3 < 2048 // STEP)
        def _():
            load_mask(i + 3).start()

    pl.semaphore_wait(barrier, len(others))

    to_xm, to_xp, to_z = (xm, zl, y, zh, co), (xp, zl, y, zh, co), (x, 1 - zl, y, zh, co)
    routes = {"X%d" % s: (rraw.at[s], rb.at[4 + s], to_xm) for s in range(NS)}
    pieces = ((0, 0, 128), (0, 128, 128), (1, 0, 128), (1, 128, 128), (3, 96, 80), (3, 176, 80))
    at = 0
    for i, (s, row, rows) in enumerate(pieces):
        kept, rows = pl.ds(at, rows), pl.ds(row, rows)
        at += pieces[i][2]
        routes["R%d" % i] = (rraw.at[s, rows], rel.at[kept], to_xp)
        routes["S%d" % i] = (rel.at[kept], rb.at[8 + s, rows], to_xp)
    routes["Y0"] = (rb.at[6], rb.at[10], to_xm)
    routes["Y1"] = (rb.at[7, pl.ds(0, 96)], rb.at[11, pl.ds(0, 96)], to_xm)
    for i, (t, rows) in enumerate(((0, pl.ds(0, 1024)), (0, pl.ds(1024, 1024)),
                                   (1, pl.ds(0, 1024)), (1, pl.ds(1024, 1024)))):
        routes["Z%d" % i] = (lraw.at[t, rows], lb.at[NT + t, rows], to_z)
    flow = {name: remote(src, dst, xs.at[i], xr.at[i], dev)
            for i, (name, (src, dst, dev)) in enumerate(routes.items())}

    def arrive(*names):
        for name in names:
            flow[name].wait_recv()

    def start(*names):
        for name in names:
            flow[name].start()

    start("X0", "R0", "R1")

    partners = [(x, zl, y, 1 - zh, co), (x, zl, y, zh, 1 - co),
                (x, zl, y + 1 - 2 * (y % 2), zh, co), (x, zl, 3 - y, zh, co)]
    colsq = acc[...].sum(axis=0, keepdims=True)
    sums = []
    for i, dev in enumerate(partners):
        cs[i] = colsq
        c = remote(cs.at[i], cr.at[i], css.at[i], csr.at[i], dev)
        c.start()
        c.wait_recv()
        sums.append(c)
        colsq = colsq + cr[i]
        if i == 0:
            start("Z0")
    divisor = jnp.minimum(jnp.sqrt(colsq + 1.0), jnp.sqrt(jnp.float32(32768.0)))
    wrow[0] = scale_ref[...] / divisor
    weights = [remote(wrow.at[0], wrow.at[1], ws.at[0], wr.at[0], to_xm),
               remote(wrow.at[0], wrow.at[2], ws.at[1], wr.at[1], (xo, zl, y, zh, co)),
               remote(wrow.at[0], wrow.at[3], ws.at[2], wr.at[2], to_z)]
    for w in weights:
        w.start()
    start("X1", "Z1", "Z2", "Z3", "X2", "X3")

    def turn_weights(i):
        wcol[i] = jnp.broadcast_to(wrow[i], (128, 1024)).T

    def scale_rb(src, dst, s, i, first=0):
        @pl.loop(first, 16)
        def _(r):
            pc, py, ph = r // 8, (r // 2) % 4, r % 2
            j = pl.multiple_of(py * 256 + ph * 128 + pc * 64 + s * 16, 16)
            rows = pl.ds(pl.multiple_of(r * 16, 16), 16)
            by = jnp.concatenate([wcol[i, pl.ds(j, 16)]] * 16, axis=1)
            dst[rows] = (src[rows].astype(f32) * by).astype(bf16)

    def scale_lb(src, dst, t, i):
        by = wrow[i, :, t * 512:(t + 1) * 512]

        @pl.loop(0, 16)
        def _(n):
            rows = pl.ds(pl.multiple_of(n * 128, 128), 128)
            dst[rows] = (src[rows].astype(f32) * by).astype(bf16)

    def scale_x1(s):
        scale_rb(rb.at[4 + s], rb.at[4 + s], s, 1)

    def scale_x2(s, first=0):
        scale_rb(rb.at[8 + s], rb.at[8 + s], s, 2, first)

    def scale_z(t):
        scale_lb(lb.at[NT + t], lb.at[NT + t], t, 3)

    other_half = (1 - co) * 128
    own_half = co * 128

    def d2_copy(n, slot):
        return remote(part.at[slot, pl.ds(other_half, 128)], d2.at[slot], ds.at[slot], dr.at[slot],
                      (x, zl, y, zh, 1 - co))

    far = (own_half + yo * 32, own_half + yo * 32 + 16)
    near = (own_half + yp * 32, own_half + ym * 32)
    via = (own_half + yp * 32, own_half + ym * 32 + 16)
    neighbours = ((x, zl, yp, zh, co), (x, zl, ym, zh, co))

    def y1_copies(n, slot, narrow):
        return [remote(h1.at[slot, d] if narrow else part.at[slot, pl.ds(far[d], 16)],
                       g1.at[n - WIDE, d] if narrow else y1.at[n, d],
                       y1s.at[slot, d], y1r.at[n, d], neighbours[d]) for d in range(2)]

    def y2_copies(n, slot, narrow):
        return [remote(h2.at[slot, d] if narrow else part.at[slot, pl.ds(near[d], 32)],
                       g2.at[n - WIDE, d] if narrow else y2.at[n, d],
                       y2s.at[slot, d], y2r.at[n, d], neighbours[d]) for d in range(2)]

    def place(out, b, s, t):
        left = b // 3
        k = 2 * (b - 3 * left) + left
        return out.at[k, pl.ds(pl.multiple_of(s * 16, 16), 16),
                      pl.ds(pl.multiple_of(t * 512, 512), 512)]

    def z1_copy(n, item):
        return remote(zs.at[n, pl.ds((1 - zh) * 16, 16)], place(out_far, *item), z1s.at[n],
                      z1r.at[n], (x, (zl + item[0] // 3) % 2, y, 1 - zh, co))

    def za_copy(n, item):
        return remote(zs.at[n, pl.ds(zh * 16, 16)], place(out_near, *item), zas.at[n],
                      zar.at[n], to_z)

    def multiply(first, count, _narrow):
        @pl.loop(first, first + count)
        def _(n):
            b, s, t = item_of(n)
            left = b // 3
            right = b - 3 * left + left * (1 - zl)
            slot = n % RING
            part[slot] = jnp.dot(rb[right * 4 + s], lb[left * NT + t],
                                 preferred_element_type=jnp.float32)
            d2_copy(n, slot).start()

    def add_core(first, count, narrow):
        @pl.loop(first, first + count)
        def _(n):
            slot = n % RING
            d2_copy(n, slot).wait()
            rows = pl.ds(own_half, 128)
            part[slot, rows] = part[slot, rows] + d2[slot]
            for d, c in enumerate(y1_copies(n, slot, narrow)):
                if narrow:
                    h1[slot, d] = part[slot, pl.ds(far[d], 16)].astype(bf16)
                c.start()

    def add_y1(first, count, narrow):
        @pl.loop(first, first + count)
        def _(n):
            slot = n % RING
            for c in y1_copies(n, slot, narrow):
                c.wait()
            for d in range(2):
                rows = pl.ds(via[d], 16)
                came = g1[n - WIDE, d].astype(f32) if narrow else y1[n, d]
                part[slot, rows] = part[slot, rows] + came
            for d, c in enumerate(y2_copies(n, slot, narrow)):
                if narrow:
                    h2[slot, d] = part[slot, pl.ds(near[d], 32)].astype(bf16)
                c.start()

    def add_y2(first, count, narrow):
        @pl.loop(first, first + count)
        def _(n):
            slot = n % RING
            item = item_of(n)
            left = item[0] // 3
            for c in y2_copies(n, slot, narrow):
                c.wait()
            total = part[slot, pl.ds(own_half + y * 32, 32)]
            for d in range(2):
                total = total + (g2[n - WIDE, d].astype(f32) if narrow else y2[n, d])
            zs[n] = total
            z1_copy(n, item).start()

            @pl.when(left == 1)
            def _():
                za_copy(n, item).start()

            @pl.when(left == 0)
            def _():
                place(out_near, *item)[...] = zs[n, pl.ds(zh * 16, 16)]

    firsts = [sum(len(p) for p in PHASES[:g]) for g in range(len(PHASES))]

    def stages(text):
        for word in re.findall("[CDEF][0-9]+", text):
            stage = {"C": multiply, "D": add_core, "E": add_y1, "F": add_y2}[word[0]]
            g = int(word[1:])
            stage(firsts[g], len(PHASES[g]), g >= NARROW)

    turn_weights(0)
    for t in range(NT):
        scale_lb(lraw.at[t], lb.at[t], t, 0)
    scale_rb(rraw.at[0], rb.at[0], 0, 0)
    scale_rb(rraw.at[1], rb.at[1], 1, 0)
    stages("C0D0")
    arrive("R0")
    start("S0", "R2")
    scale_rb(rraw.at[2], rb.at[2], 2, 0)
    scale_rb(rraw.at[3], rb.at[3], 3, 0)
    stages("C1D1E0")
    arrive("R1")
    start("S1", "R3")
    arrive("X0")
    weights[0].wait_recv()
    turn_weights(1)
    scale_x1(0)
    stages("C2D2E1F0E2F1F2")
    arrive("X1")
    scale_x1(1)
    stages("C3D3")
    weights[2].wait_recv()
    arrive("R2")
    start("S2", "R4")
    arrive("Z0", "Z1")
    scale_z(0)
    stages("C4D4E3")
    weights[1].wait_recv()
    turn_weights(2)
    arrive("S0", "S1")
    scale_x2(0)
    stages("C5D5E4F3E5F4F5")
    arrive("R3")
    start("S3", "R5")
    arrive("X2")
    scale_x1(2)
    start("Y0")
    stages("C6D6E6F6")
    arrive("R4")
    start("S4")
    arrive("X3")
    scale_x1(3)
    start("Y1")
    stages("C7D7")
    arrive("Z2", "Z3")
    scale_z(1)
    stages("C8E7D8")
    arrive("S2", "S3")
    scale_x2(1)
    stages("C9D9C10D10")
    arrive("R5")
    start("S5")
    stages("E8E9E10F7")
    arrive("Y0")
    stages("C11D11F8F9F10E11")
    arrive("Y1", "S4", "S5")
    scale_x2(3, 6)
    stages("C12C13D12D13F11E12E13")
    stages("F12F13")
    for n, item in enumerate(ITEMS):
        z1_copy(n, item).wait()
        if item[0] >= 3:
            za_copy(n, item).wait()
    for c in list(flow.values()) + sums + weights:
        c.wait_send()


def on_device(data, column_scale, keep_mask):
    dma = pltpu.SemaphoreType.DMA
    f32, bf16 = jnp.float32, jnp.bfloat16
    near, far = pl.pallas_call(
        kernel,
        out_shape=[pltpu.VMEM((5, 64, 1024), f32)] * 2,
        in_specs=[pl.BlockSpec(memory_space=pl.ANY)] * 2
        + [pl.BlockSpec(memory_space=pltpu.VMEM)],
        out_specs=[pl.BlockSpec(memory_space=pltpu.VMEM)] * 2,
        scratch_shapes=[
            pltpu.VMEM((2 * NT, 2048, 512), bf16),
            pltpu.VMEM((12, 256, 2048), bf16),
            pltpu.VMEM((NT, 2048, 512), bf16),
            pltpu.VMEM((NS, 256, 2048), bf16),
            pltpu.VMEM((672, 2048), bf16),
            pltpu.VMEM((RING, 256, 512), f32),
            pltpu.VMEM((RING, 128, 512), f32),
            pltpu.VMEM((WIDE, 2, 16, 512), f32),
            pltpu.VMEM((WIDE, 2, 32, 512), f32),
            pltpu.VMEM((RING, 2, 16, 512), bf16),
            pltpu.VMEM((N - WIDE, 2, 16, 512), bf16),
            pltpu.VMEM((RING, 2, 32, 512), bf16),
            pltpu.VMEM((N - WIDE, 2, 32, 512), bf16),
            pltpu.VMEM((N, 32, 512), f32),
            pltpu.VMEM((3, STEP, 1024), jnp.int32),
            pltpu.VMEM((8, 1024), f32),
            pltpu.VMEM((4, 1, 1024), f32),
            pltpu.VMEM((4, 1, 1024), f32),
            pltpu.VMEM((4, 1, 1024), f32),
            pltpu.VMEM((3, 1024, 128), f32),
            dma((2048 // STEP, NT + 1)), dma((4,)), dma((4,)), dma((3,)), dma((3,)),
            dma((22,)), dma((22,)), dma((RING,)), dma((RING,)),
            dma((RING, 2)), dma((N, 2)), dma((RING, 2)), dma((N, 2)),
            dma((N,)), dma((N,)), dma((N,)), dma((N,)),
        ],
        compiler_params=pltpu.CompilerParams(
            collective_id=0, has_side_effects=True, vmem_limit_bytes=61 * 2**20),
    )(data, keep_mask, column_scale.reshape(1, 1024))
    return (near + far).transpose(2, 0, 1)


def solution(mesh):
    split = Mesh(mesh.devices.reshape(4, 2, 4, 2, 2), AXES)
    return jax.shard_map(
        on_device,
        mesh=split,
        in_specs=(P(ROW, ("x", "zl")), P(("x", "zl")), P(ROW, ("x", "zl"))),
        out_specs=P(("x", "zl"), None, ROW),
        check_vma=False,
    )
```

```python
import re

import jax
import jax.numpy as jnp
from jax import lax
from jax.experimental import pallas as pl
from jax.experimental.pallas import tpu as pltpu
from jax.sharding import Mesh
from jax.sharding import PartitionSpec as P

AXES = ("x", "zl", "y", "zh", "co")
ROW = ("y", "zh", "co")
NS = 4
NT = 2

PHASES = (
    [(0, 0, 0), (0, 0, 1), (0, 1, 0), (0, 1, 1)],
    [(0, 2, 0), (0, 2, 1), (0, 3, 0), (0, 3, 1)],
    [(1, 0, 0), (1, 0, 1)],
    [(1, 1, 0), (1, 1, 1)],
    [(3, 0, 0), (3, 1, 0)],
    [(2, 0, 0), (2, 0, 1), (4, 0, 0)],
    [(1, 2, 0), (1, 2, 1), (3, 2, 0)],
    [(1, 3, 0), (1, 3, 1), (3, 3, 0)],
    [(3, 0, 1), (3, 1, 1), (3, 2, 1), (3, 3, 1)],
    [(4, 0, 1), (2, 1, 0), (2, 1, 1)],
    [(4, 1, 0), (4, 1, 1)],
    [(2, 2, 0), (2, 2, 1), (4, 2, 0), (4, 2, 1)],
    [(4, 3, 0), (4, 3, 1)],
    [(2, 3, 0), (2, 3, 1)],
)
ITEMS = [item for phase in PHASES for item in phase]
N = len(ITEMS)
RING = 16
NARROW = 9
WIDE = sum(len(phase) for phase in PHASES[:NARROW])
STEP = 256
MASKS = 6
CODES = [b * 8 + s * 2 + t for b, s, t in ITEMS]
WORDS = [sum(c << (6 * i) for i, c in enumerate(CODES[g:g + 5])) for g in range(0, N, 5)]


def item_of(n):
    group = n // 5
    word = sum(jnp.where(group == g, jnp.int32(w), 0) for g, w in enumerate(WORDS))
    code = lax.shift_right_logical(word, 6 * (n % 5)) % 64
    return code // 8, (code // 2) % 4, code % 2


def kernel(data_hbm, mask_hbm, scale_ref, out_near, out_far, lb, rb, lraw, rraw, rel, part, d2, y1, y2,
           h1, g1, h2, g2, zs, mask, acc, cs, cr, wrow, wcol, in_sem, css, csr, ws, wr, xs, xr,
           ds, dr, y1s, y1r, y2s, y2r, zsem):
    x, zl, y, zh, co = (lax.axis_index(a) for a in AXES)
    xm, xp = (x + 3) % 4, (x + 1) % 4
    xo = (x + 2) % 4
    ym, yp, yo = (y + 3) % 4, (y + 1) % 4, (y + 2) % 4
    f32, bf16 = jnp.float32, jnp.bfloat16

    def remote(src, dst, send, recv, dev):
        return pltpu.make_async_remote_copy(
            src_ref=src, dst_ref=dst, send_sem=send, recv_sem=recv,
            device_id=dev, device_id_type=pl.DeviceIdType.MESH)

    def load_mask(i):
        rows = pl.ds(pl.multiple_of(i * STEP, STEP), STEP)
        return pltpu.make_async_copy(mask_hbm.at[rows], mask.at[i % MASKS], in_sem.at[i, NT])

    def load_data(i):
        rows = pl.ds(pl.multiple_of(i * STEP, STEP), STEP)
        return [pltpu.make_async_copy(data_hbm.at[rows, t * 512:(t + 1) * 512],
                                      lraw.at[t, rows], in_sem.at[i, t]) for t in range(NT)]

    @pl.loop(0, 2048 // STEP)
    def _(i):
        for c in load_data(i):
            c.start()

        @pl.when(i < MASKS)
        def _():
            load_mask(i).start()

    barrier = pltpu.get_barrier_semaphore()
    others = [(x, zl, y, zh, 1 - co), (x, zl, yp, zh, co), (x, zl, ym, zh, co),
              (x, zl, y, 1 - zh, co), (x, 1 - zl, y, zh, co), (x, 1 - zl, y, 1 - zh, co),
              (xm, zl, y, zh, co), (xp, zl, y, zh, co), (xo, zl, y, zh, co)]
    for dev in others:
        pl.semaphore_signal(barrier, inc=1, device_id=dev, device_id_type=pl.DeviceIdType.MESH)

    acc[...] = jnp.zeros((8, 1024), f32)

    def take(i):
        load_mask(i).wait()
        for c in load_data(i):
            c.wait()
        rows = pl.ds(pl.multiple_of(i * STEP, STEP), STEP)
        for t in range(NT):
            lanes = slice(t * 512, (t + 1) * 512)
            given = lraw[t, rows].astype(f32)
            values = given * scale_ref[:, lanes]
            acc[:, lanes] += (values * values).reshape(STEP // 8, 8, 512).sum(axis=0)
            kept = (given * mask[i % MASKS, :, lanes].astype(f32)).astype(bf16)
            lraw[t, rows] = kept
            turned = kept.T
            for g in range(32):
                j = t * 32 + g
                py, ph, pc, s = j // 16, (j // 8) % 2, (j // 4) % 2, j % 4
                rraw[s, pl.ds(pc * 128 + py * 32 + ph * 16, 16), rows] = turned[g * 16:(g + 1) * 16]

        @pl.when(i + MASKS < 2048 // STEP)
        def _():
            load_mask(i + MASKS).start()

    pl.loop(0, 1024 // STEP)(take)
    pl.semaphore_wait(barrier, len(others))

    to_xm, to_xp, to_z = (xm, zl, y, zh, co), (xp, zl, y, zh, co), (x, 1 - zl, y, zh, co)
    routes = {"X%d" % s: (rraw.at[s], rb.at[4 + s], to_xm) for s in range(1, NS)}
    for i, lanes in enumerate((pl.ds(0, 1024), pl.ds(1024, 1024))):
        routes["X%d" % (4 * i)] = (rraw.at[0, :, lanes], rb.at[4, :, lanes], to_xm)
        rows = pl.ds(0, 128)
        routes["R%d" % (6 * i)] = (rraw.at[0, rows, lanes], rel.at[rows, lanes], to_xp)
    pieces = ((0, 0, 128), (0, 128, 128), (1, 0, 128), (1, 128, 128), (3, 96, 80), (3, 176, 80))
    at = 0
    for i, (s, row, rows) in enumerate(pieces):
        kept, rows = pl.ds(at, rows), pl.ds(row, rows)
        at += pieces[i][2]
        if i > 0:
            routes["R%d" % i] = (rraw.at[s, rows], rel.at[kept], to_xp)
        routes["S%d" % i] = (rel.at[kept], rb.at[8 + s, rows], to_xp)
    routes["Y0"] = (rb.at[6], rb.at[10], to_xm)
    routes["Y1"] = (rb.at[7, pl.ds(0, 96)], rb.at[11, pl.ds(0, 96)], to_xm)
    for i, (t, rows) in enumerate(((0, pl.ds(0, 1024)), (0, pl.ds(1024, 1024)),
                                   (1, pl.ds(0, 1024)), (1, pl.ds(1024, 1024)))):
        routes["Z%d" % i] = (lraw.at[t, rows], lb.at[NT + t, rows], to_z)
    flow = {name: remote(src, dst, xs.at[i], xr.at[i], dev)
            for i, (name, (src, dst, dev)) in enumerate(routes.items())}

    def arrive(*names):
        for name in names:
            flow[name].wait_recv()

    def start(*names):
        for name in names:
            flow[name].start()

    start("X0", "R0")
    pl.loop(1024 // STEP, 2048 // STEP)(take)
    start("X4", "R6", "R1")

    partners = [(x, zl, y, 1 - zh, co), (x, zl, y, zh, 1 - co),
                (x, zl, y + 1 - 2 * (y % 2), zh, co), (x, zl, 3 - y, zh, co)]
    colsq = acc[...].sum(axis=0, keepdims=True)
    sums = []
    for i, dev in enumerate(partners):
        cs[i] = colsq
        c = remote(cs.at[i], cr.at[i], css.at[i], csr.at[i], dev)
        c.start()
        c.wait_recv()
        sums.append(c)
        colsq = colsq + cr[i]
        if i == 0:
            start("Z0")
    divisor = jnp.minimum(jnp.sqrt(colsq + 1.0), jnp.sqrt(jnp.float32(32768.0)))
    wrow[0] = scale_ref[...] / divisor
    weights = [remote(wrow.at[0], wrow.at[1], ws.at[0], wr.at[0], to_xm),
               remote(wrow.at[0], wrow.at[2], ws.at[1], wr.at[1], (xo, zl, y, zh, co)),
               remote(wrow.at[0], wrow.at[3], ws.at[2], wr.at[2], to_z)]
    for w in weights:
        w.start()
    start("X1", "Z1", "Z2", "Z3", "X2", "X3")

    def turn_weights(i):
        wcol[i] = jnp.broadcast_to(wrow[i], (128, 1024)).T

    def scale_rb(src, dst, s, i, first=0):
        @pl.loop(first, 16)
        def _(r):
            pc, py, ph = r // 8, (r // 2) % 4, r % 2
            j = pl.multiple_of(py * 256 + ph * 128 + pc * 64 + s * 16, 16)
            rows = pl.ds(pl.multiple_of(r * 16, 16), 16)
            by = jnp.concatenate([wcol[i, pl.ds(j, 16)]] * 16, axis=1)
            dst[rows] = (src[rows].astype(f32) * by).astype(bf16)

    def scale_lb(src, dst, t, i):
        by = wrow[i, :, t * 512:(t + 1) * 512]

        @pl.loop(0, 16)
        def _(n):
            rows = pl.ds(pl.multiple_of(n * 128, 128), 128)
            dst[rows] = (src[rows].astype(f32) * by).astype(bf16)

    def scale_x1(s):
        scale_rb(rb.at[4 + s], rb.at[4 + s], s, 1)

    def scale_x2(s, first=0):
        scale_rb(rb.at[8 + s], rb.at[8 + s], s, 2, first)

    def scale_z(t):
        scale_lb(lb.at[NT + t], lb.at[NT + t], t, 3)

    other_half = (1 - co) * 128
    own_half = co * 128

    def d2_copy(n, slot):
        return remote(part.at[slot, pl.ds(other_half, 128)], d2.at[slot], ds.at[slot], dr.at[slot],
                      (x, zl, y, zh, 1 - co))

    far = (own_half + yo * 32, own_half + yo * 32 + 16)
    near = (own_half + yp * 32, own_half + ym * 32)
    via = (own_half + yp * 32, own_half + ym * 32 + 16)
    neighbours = ((x, zl, yp, zh, co), (x, zl, ym, zh, co))

    def y1_copies(n, slot, narrow):
        return [remote(h1.at[slot, d] if narrow else part.at[slot, pl.ds(far[d], 16)],
                       g1.at[n - WIDE, d] if narrow else y1.at[slot, d],
                       y1s.at[slot, d], y1r.at[slot, d], neighbours[d]) for d in range(2)]

    def y2_copies(n, slot, narrow):
        return [remote(h2.at[slot, d] if narrow else part.at[slot, pl.ds(near[d], 32)],
                       g2.at[n - WIDE, d] if narrow else y2.at[slot, d],
                       y2s.at[slot, d], y2r.at[slot, d], neighbours[d]) for d in range(2)]

    def place(out, b, s, t):
        left = b // 3
        k = 2 * (b - 3 * left) + left
        return out.at[k, pl.ds(pl.multiple_of(s * 16, 16), 16),
                      pl.ds(pl.multiple_of(t * 512, 512), 512)]

    def z1_copy(n, item):
        return remote(zs.at[n, pl.ds((1 - zh) * 16, 16)], place(out_far, *item), zsem.at[0],
                      zsem.at[1], (x, (zl + item[0] // 3) % 2, y, 1 - zh, co))

    def za_copy(n, item):
        return remote(zs.at[n, pl.ds(zh * 16, 16)], place(out_near, *item), zsem.at[2],
                      zsem.at[3], to_z)

    def multiply(first, count, _narrow):
        @pl.loop(first, first + count)
        def _(n):
            b, s, t = item_of(n)
            left = b // 3
            right = b - 3 * left + left * (1 - zl)
            slot = n % RING
            part[slot] = jnp.dot(rb[right * 4 + s], lb[left * NT + t],
                                 preferred_element_type=jnp.float32)
            d2_copy(n, slot).start()

    def add_core(first, count, narrow):
        @pl.loop(first, first + count)
        def _(n):
            slot = n % RING
            d2_copy(n, slot).wait()
            rows = pl.ds(own_half, 128)
            part[slot, rows] = part[slot, rows] + d2[slot]
            for d, c in enumerate(y1_copies(n, slot, narrow)):
                if narrow:
                    h1[slot, d] = part[slot, pl.ds(far[d], 16)].astype(bf16)
                c.start()

    def add_y1(first, count, narrow):
        @pl.loop(first, first + count)
        def _(n):
            slot = n % RING
            for c in y1_copies(n, slot, narrow):
                c.wait()
            for d in range(2):
                rows = pl.ds(via[d], 16)
                came = g1[n - WIDE, d].astype(f32) if narrow else y1[slot, d]
                part[slot, rows] = part[slot, rows] + came
            for d, c in enumerate(y2_copies(n, slot, narrow)):
                if narrow:
                    h2[slot, d] = part[slot, pl.ds(near[d], 32)].astype(bf16)
                c.start()

    def add_y2(first, count, narrow):
        @pl.loop(first, first + count)
        def _(n):
            slot = n % RING
            item = item_of(n)
            left = item[0] // 3
            for c in y2_copies(n, slot, narrow):
                c.wait()
            total = part[slot, pl.ds(own_half + y * 32, 32)]
            for d in range(2):
                total = total + (g2[n - WIDE, d].astype(f32) if narrow else y2[slot, d])
            zs[n] = total
            z1_copy(n, item).start()

            @pl.when(left == 1)
            def _():
                za_copy(n, item).start()

            @pl.when(left == 0)
            def _():
                place(out_near, *item)[...] = zs[n, pl.ds(zh * 16, 16)]

    firsts = [sum(len(p) for p in PHASES[:g]) for g in range(len(PHASES))]

    def stages(text):
        for word in re.findall("[CDEF][0-9]+", text):
            stage = {"C": multiply, "D": add_core, "E": add_y1, "F": add_y2}[word[0]]
            g = int(word[1:])
            stage(firsts[g], len(PHASES[g]), g >= NARROW)

    turn_weights(0)
    for t in range(NT):
        scale_lb(lraw.at[t], lb.at[t], t, 0)
    scale_rb(rraw.at[0], rb.at[0], 0, 0)
    scale_rb(rraw.at[1], rb.at[1], 1, 0)
    stages("C0D0")
    arrive("R0", "R6")
    start("S0", "R2")
    scale_rb(rraw.at[2], rb.at[2], 2, 0)
    scale_rb(rraw.at[3], rb.at[3], 3, 0)
    stages("C1D1E0")
    arrive("R1")
    start("S1", "R3")
    arrive("X0", "X4")
    weights[0].wait_recv()
    turn_weights(1)
    scale_x1(0)
    stages("C2D2E1F0E2F1F2")
    arrive("X1")
    scale_x1(1)
    stages("C3D3")
    weights[2].wait_recv()
    arrive("R2")
    start("S2", "R4")
    arrive("Z0", "Z1")
    scale_z(0)
    stages("C4D4E3")
    weights[1].wait_recv()
    turn_weights(2)
    arrive("S0", "S1")
    scale_x2(0)
    stages("C5D5E4F3E5F4F5")
    arrive("R3")
    start("S3", "R5")
    arrive("X2")
    scale_x1(2)
    start("Y0")
    stages("C6D6E6F6")
    arrive("R4")
    start("S4")
    arrive("X3")
    scale_x1(3)
    start("Y1")
    stages("C7D7")
    arrive("Z2", "Z3")
    scale_z(1)
    stages("C8E7D8")
    arrive("S2", "S3")
    scale_x2(1)
    stages("C9D9C10D10")
    arrive("R5")
    start("S5")
    stages("E8E9E10F7")
    arrive("Y0")
    stages("C11D11F8F9F10E11")
    arrive("Y1", "S4", "S5")
    scale_x2(3, 6)
    stages("C12C13D12D13F11E12E13")
    stages("F12F13")
    remote(out_far, out_far, zsem.at[0], zsem.at[1], to_z).wait()
    some = out_near.at[pl.ds(0, 2)]
    remote(some, some, zsem.at[2], zsem.at[3], to_z).wait()
    for c in list(flow.values()) + sums + weights:
        c.wait_send()


def on_device(data, column_scale, keep_mask):
    dma = pltpu.SemaphoreType.DMA
    f32, bf16 = jnp.float32, jnp.bfloat16
    near, far = pl.pallas_call(
        kernel,
        out_shape=[pltpu.VMEM((5, 64, 1024), f32)] * 2,
        in_specs=[pl.BlockSpec(memory_space=pl.ANY)] * 2
        + [pl.BlockSpec(memory_space=pltpu.VMEM)],
        out_specs=[pl.BlockSpec(memory_space=pltpu.VMEM)] * 2,
        scratch_shapes=[
            pltpu.VMEM((2 * NT, 2048, 512), bf16),
            pltpu.VMEM((12, 256, 2048), bf16),
            pltpu.VMEM((NT, 2048, 512), bf16),
            pltpu.VMEM((NS, 256, 2048), bf16),
            pltpu.VMEM((672, 2048), bf16),
            pltpu.VMEM((RING, 256, 512), f32),
            pltpu.VMEM((RING, 128, 512), f32),
            pltpu.VMEM((RING, 2, 16, 512), f32),
            pltpu.VMEM((RING, 2, 32, 512), f32),
            pltpu.VMEM((RING, 2, 16, 512), bf16),
            pltpu.VMEM((N - WIDE, 2, 16, 512), bf16),
            pltpu.VMEM((RING, 2, 32, 512), bf16),
            pltpu.VMEM((N - WIDE, 2, 32, 512), bf16),
            pltpu.VMEM((N, 32, 512), f32),
            pltpu.VMEM((MASKS, STEP, 1024), jnp.int32),
            pltpu.VMEM((8, 1024), f32),
            pltpu.VMEM((4, 1, 1024), f32),
            pltpu.VMEM((4, 1, 1024), f32),
            pltpu.VMEM((4, 1, 1024), f32),
            pltpu.VMEM((3, 1024, 128), f32),
            dma((2048 // STEP, NT + 1)), dma((4,)), dma((4,)), dma((3,)), dma((3,)),
            dma((24,)), dma((24,)), dma((RING,)), dma((RING,)),
            dma((RING, 2)), dma((RING, 2)), dma((RING, 2)), dma((RING, 2)), dma((4,)),
        ],
        compiler_params=pltpu.CompilerParams(
            collective_id=0, has_side_effects=True, vmem_limit_bytes=61 * 2**20),
    )(data, keep_mask, column_scale.reshape(1, 1024))
    return (near + far).transpose(2, 0, 1)


def solution(mesh):
    split = Mesh(mesh.devices.reshape(4, 2, 4, 2, 2), AXES)
    return jax.shard_map(
        on_device,
        mesh=split,
        in_specs=(P(ROW, ("x", "zl")), P(("x", "zl")), P(ROW, ("x", "zl"))),
        out_specs=P(("x", "zl"), None, ROW),
        check_vma=False,
    )
```

```python
import re

import jax
import jax.numpy as jnp
from jax import lax
from jax.experimental import pallas as pl
from jax.experimental.pallas import tpu as pltpu
from jax.sharding import Mesh
from jax.sharding import PartitionSpec as P

AXES = ("x", "zl", "y", "zh", "co")
ROW = ("y", "zh", "co")
NS = 4
NT = 2

PHASES = (
    [(0, 0, 0), (0, 0, 1), (0, 1, 0), (0, 1, 1)],
    [(0, 2, 0), (0, 2, 1), (0, 3, 0), (0, 3, 1)],
    [(1, 0, 0), (1, 0, 1)],
    [(1, 1, 0), (1, 1, 1)],
    [(3, 0, 0), (3, 1, 0)],
    [(2, 0, 0), (2, 0, 1), (4, 0, 0)],
    [(1, 2, 0), (1, 2, 1), (3, 2, 0)],
    [(1, 3, 0), (1, 3, 1), (3, 3, 0)],
    [(3, 0, 1), (3, 1, 1), (3, 2, 1), (3, 3, 1)],
    [(4, 0, 1), (2, 1, 0), (2, 1, 1)],
    [(4, 1, 0), (4, 1, 1)],
    [(2, 2, 0), (2, 2, 1), (4, 2, 0), (4, 2, 1)],
    [(4, 3, 0), (4, 3, 1)],
    [(2, 3, 0), (2, 3, 1)],
)
ITEMS = [item for phase in PHASES for item in phase]
N = len(ITEMS)
RING = 16
NARROW = 9
WIDE = sum(len(phase) for phase in PHASES[:NARROW])
STEP = 256
MASKS = 6
CODES = [b * 8 + s * 2 + t for b, s, t in ITEMS]
WORDS = [sum(c << (6 * i) for i, c in enumerate(CODES[g:g + 5])) for g in range(0, N, 5)]


def item_of(n):
    group = n // 5
    word = sum(jnp.where(group == g, jnp.int32(w), 0) for g, w in enumerate(WORDS))
    code = lax.shift_right_logical(word, 6 * (n % 5)) % 64
    return code // 8, (code // 2) % 4, code % 2


def kernel(data_hbm, mask_hbm, scale_ref, out_near, out_far, lb, rb, lraw, rraw, rel, part, d2, y1, y2,
           h1, g1, h2, g2, zs, mask, acc, cs, cr, wrow, wcol, in_sem, css, csr, ws, wr, xs, xr,
           ds, dr, y1s, y1r, y2s, y2r, zsem):
    x, zl, y, zh, co = (lax.axis_index(a) for a in AXES)
    xm, xp = (x + 3) % 4, (x + 1) % 4
    xo = (x + 2) % 4
    ym, yp, yo = (y + 3) % 4, (y + 1) % 4, (y + 2) % 4
    f32, bf16 = jnp.float32, jnp.bfloat16

    def remote(src, dst, send, recv, dev):
        return pltpu.make_async_remote_copy(
            src_ref=src, dst_ref=dst, send_sem=send, recv_sem=recv,
            device_id=dev, device_id_type=pl.DeviceIdType.MESH)

    def load_mask(i):
        rows = pl.ds(pl.multiple_of(i * STEP, STEP), STEP)
        return pltpu.make_async_copy(mask_hbm.at[rows], mask.at[i % MASKS], in_sem.at[i, NT])

    def load_data(i):
        rows = pl.ds(pl.multiple_of(i * STEP, STEP), STEP)
        return [pltpu.make_async_copy(data_hbm.at[rows, t * 512:(t + 1) * 512],
                                      lraw.at[t, rows], in_sem.at[i, t]) for t in range(NT)]

    barrier = pltpu.get_barrier_semaphore()
    others = [(x, zl, y, zh, 1 - co), (x, zl, yp, zh, co), (x, zl, ym, zh, co),
              (x, zl, y, 1 - zh, co), (x, 1 - zl, y, zh, co), (x, 1 - zl, y, 1 - zh, co),
              (xm, zl, y, zh, co), (xp, zl, y, zh, co), (xo, zl, y, zh, co)]
    for dev in others:
        pl.semaphore_signal(barrier, inc=1, device_id=dev, device_id_type=pl.DeviceIdType.MESH)

    @pl.loop(0, 2048 // STEP)
    def _(i):
        for c in load_data(i):
            c.start()

        @pl.when(i < MASKS)
        def _():
            load_mask(i).start()

    acc[...] = jnp.zeros((8, 1024), f32)

    def take(i):
        load_mask(i).wait()
        for c in load_data(i):
            c.wait()
        rows = pl.ds(pl.multiple_of(i * STEP, STEP), STEP)
        for t in range(NT):
            lanes = slice(t * 512, (t + 1) * 512)
            given = lraw[t, rows].astype(f32)
            values = given * scale_ref[:, lanes]
            acc[:, lanes] += (values * values).reshape(STEP // 8, 8, 512).sum(axis=0)
            kept = (given * mask[i % MASKS, :, lanes].astype(f32)).astype(bf16)
            lraw[t, rows] = kept
            turned = kept.T
            for g in range(32):
                j = t * 32 + g
                py, ph, pc, s = j // 16, (j // 8) % 2, (j // 4) % 2, j % 4
                rraw[s, pl.ds(pc * 128 + py * 32 + ph * 16, 16), rows] = turned[g * 16:(g + 1) * 16]

        @pl.when(i + MASKS < 2048 // STEP)
        def _():
            load_mask(i + MASKS).start()

    pl.loop(0, 1024 // STEP)(take)
    pl.semaphore_wait(barrier, len(others))

    to_xm, to_xp, to_z = (xm, zl, y, zh, co), (xp, zl, y, zh, co), (x, 1 - zl, y, zh, co)
    routes = {"X%d" % s: (rraw.at[s], rb.at[4 + s], to_xm) for s in range(1, NS)}
    for i, lanes in enumerate((pl.ds(0, 1024), pl.ds(1024, 1024))):
        routes["X%d" % (4 * i)] = (rraw.at[0, :, lanes], rb.at[4, :, lanes], to_xm)
        rows = pl.ds(0, 128)
        routes["R%d" % (6 * i)] = (rraw.at[0, rows, lanes], rel.at[rows, lanes], to_xp)
    pieces = ((0, 0, 128), (0, 128, 128), (1, 0, 128), (1, 128, 128), (3, 96, 80), (3, 176, 80))
    at = 0
    for i, (s, row, rows) in enumerate(pieces):
        kept, rows = pl.ds(at, rows), pl.ds(row, rows)
        at += pieces[i][2]
        if i > 0:
            routes["R%d" % i] = (rraw.at[s, rows], rel.at[kept], to_xp)
        routes["S%d" % i] = (rel.at[kept], rb.at[8 + s, rows], to_xp)
    routes["Y0"] = (rb.at[6], rb.at[10], to_xm)
    routes["Y1"] = (rb.at[7, pl.ds(0, 96)], rb.at[11, pl.ds(0, 96)], to_xm)
    for i, (t, rows) in enumerate(((0, pl.ds(256, 768)), (0, pl.ds(1024, 1024)),
                                   (1, pl.ds(0, 1024)), (1, pl.ds(1024, 1024)),
                                   (0, pl.ds(0, 256)))):
        routes["Z%d" % i] = (lraw.at[t, rows], lb.at[NT + t, rows], to_z)
    flow = {name: remote(src, dst, xs.at[i], xr.at[i], dev)
            for i, (name, (src, dst, dev)) in enumerate(routes.items())}

    def arrive(*names):
        for name in names:
            flow[name].wait_recv()

    def start(*names):
        for name in names:
            flow[name].start()

    start("X0", "R0", "Z4")
    pl.loop(1024 // STEP, 2048 // STEP)(take)
    start("X4", "R6", "R1")

    partners = [(x, zl, y, 1 - zh, co), (x, zl, y, zh, 1 - co),
                (x, zl, y + 1 - 2 * (y % 2), zh, co), (x, zl, 3 - y, zh, co)]
    colsq = acc[...].sum(axis=0, keepdims=True)
    sums = []
    for i, dev in enumerate(partners):
        cs[i] = colsq
        c = remote(cs.at[i], cr.at[i], css.at[i], csr.at[i], dev)
        c.start()
        c.wait_recv()
        sums.append(c)
        colsq = colsq + cr[i]
        if i == 0:
            start("Z0")
    divisor = jnp.minimum(jnp.sqrt(colsq + 1.0), jnp.sqrt(jnp.float32(32768.0)))
    wrow[0] = scale_ref[...] / divisor
    weights = [remote(wrow.at[0], wrow.at[1], ws.at[0], wr.at[0], to_xm),
               remote(wrow.at[0], wrow.at[2], ws.at[1], wr.at[1], (xo, zl, y, zh, co)),
               remote(wrow.at[0], wrow.at[3], ws.at[2], wr.at[2], to_z)]
    for w in weights:
        w.start()
    start("X1", "Z1", "Z2", "Z3", "X2", "X3")

    def turn_weights(i):
        wcol[i] = jnp.broadcast_to(wrow[i], (128, 1024)).T

    def scale_rb(src, dst, s, i, first=0):
        @pl.loop(first, 16)
        def _(r):
            pc, py, ph = r // 8, (r // 2) % 4, r % 2
            j = pl.multiple_of(py * 256 + ph * 128 + pc * 64 + s * 16, 16)
            rows = pl.ds(pl.multiple_of(r * 16, 16), 16)
            by = jnp.concatenate([wcol[i, pl.ds(j, 16)]] * 16, axis=1)
            dst[rows] = (src[rows].astype(f32) * by).astype(bf16)

    def scale_lb(src, dst, t, i):
        by = wrow[i, :, t * 512:(t + 1) * 512]

        @pl.loop(0, 16)
        def _(n):
            rows = pl.ds(pl.multiple_of(n * 128, 128), 128)
            dst[rows] = (src[rows].astype(f32) * by).astype(bf16)

    def scale_x1(s):
        scale_rb(rb.at[4 + s], rb.at[4 + s], s, 1)

    def scale_x2(s, first=0):
        scale_rb(rb.at[8 + s], rb.at[8 + s], s, 2, first)

    def scale_z(t):
        scale_lb(lb.at[NT + t], lb.at[NT + t], t, 3)

    other_half = (1 - co) * 128
    own_half = co * 128

    def d2_copy(n, slot):
        return remote(part.at[slot, pl.ds(other_half, 128)], d2.at[slot], ds.at[slot], dr.at[slot],
                      (x, zl, y, zh, 1 - co))

    far = (own_half + yo * 32, own_half + yo * 32 + 16)
    near = (own_half + yp * 32, own_half + ym * 32)
    via = (own_half + yp * 32, own_half + ym * 32 + 16)
    neighbours = ((x, zl, yp, zh, co), (x, zl, ym, zh, co))

    def y1_copies(n, slot, narrow):
        return [remote(h1.at[slot, d] if narrow else part.at[slot, pl.ds(far[d], 16)],
                       g1.at[n - WIDE, d] if narrow else y1.at[slot, d],
                       y1s.at[slot, d], y1r.at[slot, d], neighbours[d]) for d in range(2)]

    def y2_copies(n, slot, narrow):
        return [remote(h2.at[slot, d] if narrow else part.at[slot, pl.ds(near[d], 32)],
                       g2.at[n - WIDE, d] if narrow else y2.at[slot, d],
                       y2s.at[slot, d], y2r.at[slot, d], neighbours[d]) for d in range(2)]

    def place(out, b, s, t):
        left = b // 3
        k = 2 * (b - 3 * left) + left
        return out.at[k, pl.ds(pl.multiple_of(s * 16, 16), 16),
                      pl.ds(pl.multiple_of(t * 512, 512), 512)]

    def z1_copy(n, item):
        return remote(zs.at[n, pl.ds((1 - zh) * 16, 16)], place(out_far, *item), zsem.at[0],
                      zsem.at[1], (x, (zl + item[0] // 3) % 2, y, 1 - zh, co))

    def za_copy(n, item):
        return remote(zs.at[n, pl.ds(zh * 16, 16)], place(out_near, *item), zsem.at[2],
                      zsem.at[3], to_z)

    def multiply(first, count, _narrow):
        @pl.loop(first, first + count)
        def _(n):
            b, s, t = item_of(n)
            left = b // 3
            right = b - 3 * left + left * (1 - zl)
            slot = n % RING
            part[slot] = jnp.dot(rb[right * 4 + s], lb[left * NT + t],
                                 preferred_element_type=jnp.float32)
            d2_copy(n, slot).start()

    def add_core(first, count, narrow):
        @pl.loop(first, first + count)
        def _(n):
            slot = n % RING
            d2_copy(n, slot).wait()
            rows = pl.ds(own_half, 128)
            part[slot, rows] = part[slot, rows] + d2[slot]
            for d, c in enumerate(y1_copies(n, slot, narrow)):
                if narrow:
                    h1[slot, d] = part[slot, pl.ds(far[d], 16)].astype(bf16)
                c.start()

    def add_y1(first, count, narrow):
        @pl.loop(first, first + count)
        def _(n):
            slot = n % RING
            for c in y1_copies(n, slot, narrow):
                c.wait()
            for d in range(2):
                rows = pl.ds(via[d], 16)
                came = g1[n - WIDE, d].astype(f32) if narrow else y1[slot, d]
                part[slot, rows] = part[slot, rows] + came
            for d, c in enumerate(y2_copies(n, slot, narrow)):
                if narrow:
                    h2[slot, d] = part[slot, pl.ds(near[d], 32)].astype(bf16)
                c.start()

    def add_y2(first, count, narrow):
        @pl.loop(first, first + count)
        def _(n):
            slot = n % RING
            item = item_of(n)
            left = item[0] // 3
            for c in y2_copies(n, slot, narrow):
                c.wait()
            total = part[slot, pl.ds(own_half + y * 32, 32)]
            for d in range(2):
                total = total + (g2[n - WIDE, d].astype(f32) if narrow else y2[slot, d])
            zs[n] = total
            z1_copy(n, item).start()

            @pl.when(left == 1)
            def _():
                za_copy(n, item).start()

            @pl.when(left == 0)
            def _():
                place(out_near, *item)[...] = zs[n, pl.ds(zh * 16, 16)]

    firsts = [sum(len(p) for p in PHASES[:g]) for g in range(len(PHASES))]

    def stages(text):
        for word in re.findall("[CDEF][0-9]+", text):
            stage = {"C": multiply, "D": add_core, "E": add_y1, "F": add_y2}[word[0]]
            g = int(word[1:])
            stage(firsts[g], len(PHASES[g]), g >= NARROW)

    turn_weights(0)
    for t in range(NT):
        scale_lb(lraw.at[t], lb.at[t], t, 0)
    scale_rb(rraw.at[0], rb.at[0], 0, 0)
    scale_rb(rraw.at[1], rb.at[1], 1, 0)
    stages("C0D0")
    arrive("R0", "R6")
    start("S0", "R2")
    scale_rb(rraw.at[2], rb.at[2], 2, 0)
    scale_rb(rraw.at[3], rb.at[3], 3, 0)
    stages("C1D1E0")
    arrive("R1")
    start("S1", "R3")
    arrive("X0", "X4")
    weights[0].wait_recv()
    turn_weights(1)
    scale_x1(0)
    stages("C2D2E1F0E2F1F2")
    arrive("X1")
    scale_x1(1)
    stages("C3D3")
    weights[2].wait_recv()
    arrive("R2")
    start("S2", "R4")
    arrive("Z0", "Z1", "Z4")
    scale_z(0)
    stages("C4D4E3")
    weights[1].wait_recv()
    turn_weights(2)
    arrive("S0", "S1")
    scale_x2(0)
    stages("C5D5E4F3E5F4F5")
    arrive("R3")
    start("S3", "R5")
    arrive("X2")
    scale_x1(2)
    start("Y0")
    stages("C6D6E6F6")
    arrive("R4")
    start("S4")
    arrive("X3")
    scale_x1(3)
    start("Y1")
    stages("C7D7")
    arrive("Z2", "Z3")
    scale_z(1)
    stages("C8E7D8")
    arrive("S2", "S3")
    scale_x2(1)
    stages("C9D9C10D10")
    arrive("R5")
    start("S5")
    stages("E8E9E10F7")
    arrive("Y0")
    stages("C11D11F8F9F10E11")
    arrive("Y1", "S4", "S5")
    scale_x2(3, 6)
    stages("C12C13D12D13F11E12E13")
    stages("F12F13")
    remote(out_far, out_far, zsem.at[0], zsem.at[1], to_z).wait()
    some = out_near.at[pl.ds(0, 2)]
    remote(some, some, zsem.at[2], zsem.at[3], to_z).wait()
    for c in list(flow.values()) + sums + weights:
        c.wait_send()


def on_device(data, column_scale, keep_mask):
    dma = pltpu.SemaphoreType.DMA
    f32, bf16 = jnp.float32, jnp.bfloat16
    near, far = pl.pallas_call(
        kernel,
        out_shape=[pltpu.VMEM((5, 64, 1024), f32)] * 2,
        in_specs=[pl.BlockSpec(memory_space=pl.ANY)] * 2
        + [pl.BlockSpec(memory_space=pltpu.VMEM)],
        out_specs=[pl.BlockSpec(memory_space=pltpu.VMEM)] * 2,
        scratch_shapes=[
            pltpu.VMEM((2 * NT, 2048, 512), bf16),
            pltpu.VMEM((12, 256, 2048), bf16),
            pltpu.VMEM((NT, 2048, 512), bf16),
            pltpu.VMEM((NS, 256, 2048), bf16),
            pltpu.VMEM((672, 2048), bf16),
            pltpu.VMEM((RING, 256, 512), f32),
            pltpu.VMEM((RING, 128, 512), f32),
            pltpu.VMEM((RING, 2, 16, 512), f32),
            pltpu.VMEM((RING, 2, 32, 512), f32),
            pltpu.VMEM((RING, 2, 16, 512), bf16),
            pltpu.VMEM((N - WIDE, 2, 16, 512), bf16),
            pltpu.VMEM((RING, 2, 32, 512), bf16),
            pltpu.VMEM((N - WIDE, 2, 32, 512), bf16),
            pltpu.VMEM((N, 32, 512), f32),
            pltpu.VMEM((MASKS, STEP, 1024), jnp.int32),
            pltpu.VMEM((8, 1024), f32),
            pltpu.VMEM((4, 1, 1024), f32),
            pltpu.VMEM((4, 1, 1024), f32),
            pltpu.VMEM((4, 1, 1024), f32),
            pltpu.VMEM((3, 1024, 128), f32),
            dma((2048 // STEP, NT + 1)), dma((4,)), dma((4,)), dma((3,)), dma((3,)),
            dma((25,)), dma((25,)), dma((RING,)), dma((RING,)),
            dma((RING, 2)), dma((RING, 2)), dma((RING, 2)), dma((RING, 2)), dma((4,)),
        ],
        compiler_params=pltpu.CompilerParams(
            collective_id=0, has_side_effects=True, vmem_limit_bytes=61 * 2**20),
    )(data, keep_mask, column_scale.reshape(1, 1024))
    return (near + far).transpose(2, 0, 1)


def solution(mesh):
    split = Mesh(mesh.devices.reshape(4, 2, 4, 2, 2), AXES)
    return jax.shard_map(
        on_device,
        mesh=split,
        in_specs=(P(ROW, ("x", "zl")), P(("x", "zl")), P(ROW, ("x", "zl"))),
        out_specs=P(("x", "zl"), None, ROW),
        check_vma=False,
    )
```
